32 devices in a mesh: rows: 8 (over z, x), grp: 4 (over y, core).
Axes of the slice: x: 2, y: 2, z: 4, core: 2. Of those that a mesh axis runs over, the one named last changes fastest.
Arguments:
- tiles: bfloat16 [4096, 128, 128], P(('rows', 'grp')), may hold values from -0.3125 to 0.3125
- tile_rows: int32 [4096], P(('rows', 'grp')), may hold values from 0 to 47, as said below
- tile_cols: int32 [4096], P(('rows', 'grp')), may hold values from 0 to 511, as said below
- tile_count: int32 [32], P(('rows', 'grp')), may hold values from 32 to 128, as said below
- block_perm: int32 [512], replicated, may hold values from 0 to 511, as said below
- panel: bfloat16 [512, 128, 256], P(('rows', 'grp')), may hold values from -6 to 6
Outputs:
- sketch: bfloat16 [1536, 128, 256], P(('rows', 'grp'))
- gram: float32 [512, 128, 256], P(('rows', 'grp'))
The draws below stay inside these ranges and needn't reach their ends.
Inputs may be any that keep to these rules, and one draw needn't show every extreme that they name: `tile_rows`: each device's live tile rows are non-decreasing; slots past the count hold 47. `tile_cols`: among one device's live tiles, those whose block_perm positions lie with one owner (position // 16) name at most 2 distinct column blocks; every device reaches 2 for some owner. `tile_count`: some device has 128 live tiles. `block_perm`: A permutation of the column blocks.
All inputs are finite; a program needn't handle non-finite values.
Results may differ from the reference program's by a relative error of at most 0.0034.
Values may be sent and summed in bfloat16 or wider, within the bound.
A program may use at most 128 MiB of HBM per device.

```python
import jax
import jax.numpy as jnp
from jax import lax

BS = 128
K = 256
RB_DEV = 48
TILE_CAP = 128
CB_DEV = 16
PAIR_CAP = 2
NDEV = 32
NCB = 512


def tile_layout(key):
    base = jax.random.fold_in(key, 7)
    order = jax.random.permutation(jax.random.fold_in(base, 1), NCB).astype(jnp.int32)
    inverse = jnp.argsort(order).astype(jnp.int32)
    first_pick = jax.random.randint(jax.random.fold_in(base, 2), (NDEV, NDEV), 0, CB_DEV).astype(jnp.int32)
    step_pick = jax.random.randint(jax.random.fold_in(base, 8), (NDEV, NDEV), 0, CB_DEV - 1).astype(jnp.int32)
    second_pick = ((first_pick + 1 + step_pick) % CB_DEV).astype(jnp.int32)
    owners = jax.random.randint(jax.random.fold_in(base, 3), (NDEV, TILE_CAP), 0, NDEV).astype(jnp.int32)
    owners = owners.at[:, 1].set(owners[:, 0])
    sides = jax.random.randint(jax.random.fold_in(base, 9), (NDEV, TILE_CAP), 0, 2).astype(jnp.int32)
    sides = sides.at[:, 0].set(0).at[:, 1].set(1)
    source = jnp.arange(NDEV, dtype=jnp.int32)[:, None] + jnp.zeros((NDEV, TILE_CAP), jnp.int32)
    local = jnp.where(sides == 0, first_pick[source, owners], second_pick[source, owners])
    stores = (owners * CB_DEV + local).astype(jnp.int32)
    columns = inverse[stores].astype(jnp.int32)
    raw_rows = jax.random.randint(jax.random.fold_in(base, 4), (NDEV, TILE_CAP), 0, RB_DEV).astype(jnp.int32)
    counts = jax.random.randint(jax.random.fold_in(base, 5), (NDEV,), TILE_CAP // 4, TILE_CAP + 1).astype(jnp.int32)
    fullest = jax.random.randint(jax.random.fold_in(base, 6), (), 0, NDEV)
    counts = jnp.where(jnp.arange(NDEV) == fullest, TILE_CAP, counts).astype(jnp.int32)
    is_live = jnp.arange(TILE_CAP)[None, :] < counts[:, None]
    rows_sorted = jnp.sort(jnp.where(is_live, raw_rows, RB_DEV - 1), axis=1).astype(jnp.int32)
    return (order, columns.reshape(-1), rows_sorted.reshape(-1), counts)


def draw_tile_rows(key, part):
    return tile_layout(key)[2]


def draw_tile_cols(key, part):
    return tile_layout(key)[1]


def draw_tile_count(key, part):
    return tile_layout(key)[3]


def draw_block_perm(key, part):
    return tile_layout(key)[0]


def steps_of(own_key, dims, split, smallest, high):
    level = 1.0
    for axis_at, shards_of in split:
        steps = jax.random.uniform(jax.random.fold_in(jax.random.fold_in(own_key, 6), axis_at), (shards_of,), jnp.float32, smallest / len(split), high / len(split))
        level = level * jnp.repeat(jnp.exp(steps), dims[axis_at] // shards_of).reshape((-1,) + (1,) * (len(dims) - 1 - axis_at))
    return level


def scatter_about(own_key, dims, scale, bound, shards=(), kind=jnp.bfloat16):
    loudness = steps_of(own_key, dims, shards, -0.22, 0.18) if shards else 1.0
    array = jax.random.normal(own_key, dims, jnp.float32) * scale * loudness
    return jnp.minimum(jnp.maximum(array, -bound), bound).astype(kind)


def setup_inputs(seed: int = 0) -> dict:
    splits = jax.random.split(jax.random.key(seed), 7)
    return {
        "tiles": scatter_about(splits[0], (NDEV * TILE_CAP, BS, BS), (BS * TILE_CAP // RB_DEV) ** -0.5, 0.3125, ((0, 32),)),
        "tile_rows": draw_tile_rows(jax.random.fold_in(splits[6], 71), 0),
        "tile_cols": draw_tile_cols(jax.random.fold_in(splits[6], 71), 0),
        "tile_count": draw_tile_count(jax.random.fold_in(splits[6], 71), 0),
        "block_perm": draw_block_perm(jax.random.fold_in(splits[6], 71), 0),
        "panel": scatter_about(splits[5], (NCB, BS, K), 1.0, 6.0, ((0, 32),)),
    }


def block_ranks(stored_at, is_live):
    positions = jnp.arange(NCB, dtype=jnp.int32)
    hits = is_live[:, None] & (stored_at[:, None] == positions[None, :])
    needed = jnp.any(hits, axis=0).reshape(NDEV, CB_DEV)
    ranking = (jnp.cumsum(needed.astype(jnp.int32), axis=1) - 1).astype(jnp.int32)
    local_ids = jnp.arange(CB_DEV, dtype=jnp.int32)
    listed = [jnp.max(jnp.where(needed & (ranking == slot), local_ids[None, :], -1), axis=1) for slot in range(PAIR_CAP)]
    return ranking, jnp.stack(listed, axis=1).astype(jnp.int32)


def reference(tiles, tile_rows, tile_cols, tile_count, block_perm, panel):
    tiles_dev = tiles.reshape(NDEV, TILE_CAP, BS, BS)
    rows_dev = tile_rows.reshape(NDEV, TILE_CAP)
    cols_dev = tile_cols.reshape(NDEV, TILE_CAP)
    slot_ids = jnp.arange(TILE_CAP, dtype=jnp.int32)
    owner_ids = jnp.arange(NDEV, dtype=jnp.int32)

    def one_device(total, inputs):
        block, row_ids, col_ids, count = inputs
        is_live = slot_ids < count
        weight = jnp.where(is_live, 1.0, 0.0).astype(jnp.float32)
        stored_at = block_perm[col_ids].astype(jnp.int32)
        owner_of = (stored_at // CB_DEV).astype(jnp.int32)
        local_block = (stored_at % CB_DEV).astype(jnp.int32)
        ranking, listed = block_ranks(stored_at, is_live)
        slot_of = (owner_of * PAIR_CAP + ranking[owner_of, local_block]).astype(jnp.int32)
        slot_of = jnp.where(is_live, slot_of, 0).astype(jnp.int32)
        block_f = block.astype(jnp.float32)
        fetched = panel[stored_at].astype(jnp.float32)
        product = jnp.einsum("tij,tjk->tik", block_f, fetched)
        sketch_dev = jax.ops.segment_sum(product * weight[:, None, None], row_ids, num_segments=RB_DEV).astype(jnp.bfloat16)
        partial_value = jnp.einsum("tij,tik->tjk", block_f, sketch_dev[row_ids].astype(jnp.float32))
        per_slot = jax.ops.segment_sum(partial_value * weight[:, None, None], slot_of, num_segments=NDEV * PAIR_CAP).astype(jnp.bfloat16)
        flat_list = listed.reshape(-1)
        valid = jnp.where(flat_list >= 0, 1.0, 0.0).astype(jnp.float32)
        target = (jnp.repeat(owner_ids, PAIR_CAP) * CB_DEV + jnp.maximum(flat_list, 0)).astype(jnp.int32)
        total = total.at[target].add(per_slot.astype(jnp.float32) * valid[:, None, None])
        return total, sketch_dev

    zero_gram = jnp.zeros((NCB, BS, K), jnp.float32)
    gram, sketches = lax.scan(one_device, zero_gram, (tiles_dev, rows_dev, cols_dev, tile_count))
    return sketches.reshape(NDEV * RB_DEV, BS, K), gram
```

```python
import functools

import jax
import jax.numpy as jnp
from jax import lax
from jax.experimental import pallas as pl
from jax.experimental.pallas import tpu as pltpu
from jax.sharding import PartitionSpec as P

RB_DEV = 48
PAIR_CAP = 2
UNROLL = 4
AXES = ("rows", "grp")
VMEM_LIMIT = 60 * 1024 * 1024


def index_tables(tile_rows, tile_cols, tile_count, block_perm, devices, held):
    slots = tile_cols.shape[0]
    live = jnp.arange(slots, dtype=jnp.int32) < tile_count[0]
    blocks = jnp.arange(block_perm.shape[0], dtype=jnp.int32)
    stored = jnp.sum(jnp.where(tile_cols[:, None] == blocks[None, :], block_perm[None, :], 0), axis=1)
    owner = stored // held
    local = stored % held
    rank = jnp.any(
        live[None, :] & (owner[None, :] == owner[:, None]) & (local[None, :] < local[:, None]), axis=1
    ).astype(jnp.int32)
    mine = live[None, :] & (owner[None, :] == jnp.arange(devices, dtype=jnp.int32)[:, None])
    first = jnp.min(jnp.where(mine, local[None, :], held), axis=1)
    last = jnp.max(jnp.where(mine, local[None, :], -1), axis=1)
    wanted = jnp.stack(
        [jnp.where(last >= 0, first, -1), jnp.where(last > first, last, -1)], axis=-1
    ).astype(jnp.int32)
    slot = jnp.where(live, owner * PAIR_CAP + rank, devices * PAIR_CAP)
    row = jnp.where(live, tile_rows, RB_DEV)
    return wanted, slot.astype(jnp.int32), row.astype(jnp.int32)


def pick_kernel(asked, panel, out):
    def body(j, c):
        out[j] = panel[jnp.maximum(asked[j], 0)]
        return c

    lax.fori_loop(0, out.shape[0], body, 0, unroll=4)


def product_kernel(count, slot, row, tiles, fetched, sketch, outbound, sk, part):
    nslots = outbound.shape[0]
    steps = (count[0] + UNROLL - 1) // UNROLL

    def clear(ref):
        def body(i, c):
            ref[i] = jnp.zeros(ref.shape[1:], ref.dtype)
            return c

        lax.fori_loop(0, ref.shape[0], body, 0)

    clear(sk)
    clear(part)

    def forward(i, c):
        got = []
        for u in range(UNROLL):
            t = i * UNROLL + u
            block = fetched[jnp.minimum(slot[t], nslots - 1)]
            got.append(jnp.dot(tiles[t], block, preferred_element_type=jnp.float32))
        for u in range(UNROLL):
            r = row[i * UNROLL + u]
            sk[r] = sk[r] + got[u]
        return c

    lax.fori_loop(0, steps, forward, 0)

    def rounded(i, c):
        sketch[i] = sk[i].astype(sketch.dtype)
        return c

    lax.fori_loop(0, sketch.shape[0], rounded, 0)

    def backward(i, c):
        got = []
        for u in range(UNROLL):
            t = i * UNROLL + u
            block = sketch[jnp.minimum(row[t], sketch.shape[0] - 1)]
            got.append(
                lax.dot_general(
                    tiles[t], block, (((0,), (0,)), ((), ())), preferred_element_type=jnp.float32
                )
            )
        for u in range(UNROLL):
            s = slot[i * UNROLL + u]
            part[s] = part[s] + got[u]
        return c

    lax.fori_loop(0, steps, backward, 0)

    def send_form(i, c):
        outbound[i] = part[i].astype(outbound.dtype)
        return c

    lax.fori_loop(0, nslots, send_form, 0)


def gram_kernel(asked, inbound, gram):
    def clear(i, c):
        gram[i] = jnp.zeros(gram.shape[1:], gram.dtype)
        return c

    lax.fori_loop(0, gram.shape[0], clear, 0)

    def body(j, c):
        b = asked[j]

        @pl.when(b >= 0)
        def _():
            gram[b] = gram[b] + inbound[j].astype(jnp.float32)

        return c

    lax.fori_loop(0, inbound.shape[0], body, 0)


SMEM = pl.BlockSpec(memory_space=pltpu.SMEM)
VMEM = pl.BlockSpec(memory_space=pltpu.VMEM)


def per_device(tiles, tile_rows, tile_cols, tile_count, block_perm, panel):
    devices = lax.axis_size(AXES)
    held, depth, width = panel.shape
    nslots = devices * PAIR_CAP
    part = width if nslots <= tiles.shape[0] else width // 2
    wanted, slot, row = index_tables(tile_rows, tile_cols, tile_count, block_perm, devices, held)
    asked = lax.all_to_all(wanted, AXES, split_axis=0, concat_axis=0, tiled=True).reshape(-1)
    params = pltpu.CompilerParams(vmem_limit_bytes=VMEM_LIMIT)
    outgoing = pl.pallas_call(
        pick_kernel,
        out_shape=jax.ShapeDtypeStruct((nslots, depth, width), panel.dtype),
        in_specs=[SMEM, VMEM],
        out_specs=VMEM,
        compiler_params=params,
    )(asked, panel)
    fetched = lax.all_to_all(outgoing, AXES, split_axis=0, concat_axis=0, tiled=True)
    sketch, outbound = pl.pallas_call(
        product_kernel,
        out_shape=(
            jax.ShapeDtypeStruct((RB_DEV, depth, width), jnp.bfloat16),
            jax.ShapeDtypeStruct((nslots, depth, width), jnp.bfloat16),
        ),
        grid=(width // part,),
        in_specs=[
            SMEM,
            SMEM,
            SMEM,
            pl.BlockSpec(tiles.shape, lambda k: (0, 0, 0), pipeline_mode=pl.Buffered(1)),
            pl.BlockSpec((nslots, depth, part), lambda k: (0, 0, k), pipeline_mode=pl.Buffered(1)),
        ],
        out_specs=(
            pl.BlockSpec((RB_DEV, depth, part), lambda k: (0, 0, k), pipeline_mode=pl.Buffered(1)),
            pl.BlockSpec((nslots, depth, part), lambda k: (0, 0, k), pipeline_mode=pl.Buffered(1)),
        ),
        scratch_shapes=[
            pltpu.VMEM((RB_DEV + 1, depth, part), jnp.float32),
            pltpu.VMEM((nslots + 1, depth, part), jnp.float32),
        ],
        compiler_params=params,
    )(tile_count, slot, row, tiles, fetched.reshape(nslots, depth, width))
    inbound = lax.all_to_all(outbound, AXES, split_axis=0, concat_axis=0, tiled=True)
    gram = pl.pallas_call(
        gram_kernel,
        out_shape=jax.ShapeDtypeStruct((held, depth, width), jnp.float32),
        in_specs=[SMEM, VMEM],
        out_specs=VMEM,
        compiler_params=params,
    )(asked, inbound.reshape(nslots, depth, width))
    return sketch, gram


def solution(mesh):
    spec = P(AXES, None, None)
    return jax.shard_map(
        per_device,
        mesh=mesh,
        in_specs=(spec, P(AXES), P(AXES), P(AXES), P(), spec),
        out_specs=(spec, spec),
        check_vma=False,
    )
```

```python
import functools

import jax
import jax.numpy as jnp
from jax import lax
from jax.experimental import pallas as pl
from jax.experimental.pallas import tpu as pltpu
from jax.sharding import PartitionSpec as P

RB_DEV = 48
PAIR_CAP = 2
UNROLL = 4
AXES = ("rows", "grp")
VMEM_LIMIT = 60 * 1024 * 1024


def index_tables(tile_rows, tile_cols, tile_count, block_perm, devices, held):
    slots = tile_cols.shape[0]
    live = jnp.arange(slots, dtype=jnp.int32) < tile_count[0]
    blocks = jnp.arange(block_perm.shape[0], dtype=jnp.int32)
    stored = jnp.sum(jnp.where(tile_cols[:, None] == blocks[None, :], block_perm[None, :], 0), axis=1)
    owner = stored // held
    local = stored % held
    rank = jnp.any(
        live[None, :] & (owner[None, :] == owner[:, None]) & (local[None, :] < local[:, None]), axis=1
    ).astype(jnp.int32)
    mine = live[None, :] & (owner[None, :] == jnp.arange(devices, dtype=jnp.int32)[:, None])
    first = jnp.min(jnp.where(mine, local[None, :], held), axis=1)
    last = jnp.max(jnp.where(mine, local[None, :], -1), axis=1)
    wanted = jnp.stack(
        [jnp.where(last >= 0, first, -1), jnp.where(last > first, last, -1)], axis=-1
    ).astype(jnp.int32)
    slot = jnp.where(live, owner * PAIR_CAP + rank, devices * PAIR_CAP)
    row = jnp.where(live, tile_rows, RB_DEV)
    return wanted, slot.astype(jnp.int32), row.astype(jnp.int32)


LINE = 4
MESH = pl.DeviceIdType.MESH


class Place:
    def __init__(self, line, rows, grp):
        self.line, self.grp = line, grp
        self.plane_rows = rows // line
        self.plane = self.plane_rows * grp
        row = lax.axis_index("rows")
        self.z = row // self.plane_rows
        self.p = (row % self.plane_rows) * grp + lax.axis_index("grp")

    def device(self, z, p):
        return (z * self.plane_rows + p // self.grp, p % self.grp)

    def peer(self, i):
        return lax.rem(self.p + i, self.plane)

    def greet(self):
        barrier = pltpu.get_barrier_semaphore()
        for k in range(1, self.line):
            to = self.device(lax.rem(self.z + k, self.line), self.p)
            pl.semaphore_signal(barrier, inc=1, device_id=to, device_id_type=MESH)

        def signal(i, c):
            to = self.device(self.z, self.peer(i))
            pl.semaphore_signal(barrier, inc=1, device_id=to, device_id_type=MESH)
            return c

        lax.fori_loop(1, self.plane, signal, 0)
        pl.semaphore_wait(barrier, self.line - 1 + self.plane - 1)

    def inside(self, z):
        return (z >= 0) & (z < self.line)


def remote(src, dst, send, recv, to):
    return pltpu.make_async_remote_copy(
        src_ref=src, dst_ref=dst, send_sem=send, recv_sem=recv, device_id=to, device_id_type=MESH
    )


def fetch_kernel(line, rows, grp, wanted, panel, fetched, asked, *scratch):
    far, (ids, out, id_send, id_recv, z_send, z_recv, send, recv, local) = (
        scratch[: 2 * (line - 1)],
        scratch[2 * (line - 1) :],
    )
    at = Place(line, rows, grp)
    z, p, plane = at.z, at.p, at.plane
    at.greet()

    def unit(way, k):
        return panel if k == 0 else far[way * (line - 1) + k - 1]

    def along(way, k):
        step = 1 if way == 0 else -1
        to = at.device(jnp.clip(z + step, 0, line - 1), p)
        return remote(unit(way, k - 1), unit(way, k), z_send.at[way, k - 1], z_recv.at[way, k - 1], to)

    def source(way, k):
        return z - k if way == 0 else z + k

    def sends(way, k):
        return at.inside(z + (1 if way == 0 else -1)) & at.inside(source(way, k - 1))

    def id_copy(i, mine):
        q = at.peer(i)
        slot = p if mine else q
        return remote(wanted.at[q], asked.at[slot], id_send.at[q], id_recv.at[slot], at.device(z, q))

    def start_ids(i, c):
        id_copy(i, True).start()
        return c

    lax.fori_loop(1, plane, start_ids, 0)
    for way in range(2):
        pl.when(sends(way, 1))(lambda way=way: along(way, 1).start())
    asked[p] = wanted[p]

    def wait_ids(i, c):
        id_copy(i, False).wait()
        return c

    lax.fori_loop(1, plane, wait_ids, 0)
    to_smem = pltpu.make_async_copy(asked, ids, local)
    to_smem.start()
    to_smem.wait()

    def spread(plane_z, held):
        def pick(i, c):
            q = at.peer(i)
            for j in range(PAIR_CAP):
                block = jnp.maximum(ids[q, 0, plane_z * PAIR_CAP + j], 0)
                out[plane_z, q, j] = held[block]
            return c

        lax.fori_loop(1, plane, pick, 0)
        for j in range(PAIR_CAP):
            block = jnp.maximum(ids[p, 0, plane_z * PAIR_CAP + j], 0)
            fetched[plane_z, p, j] = held[block]

        def start(i, c):
            q = at.peer(i)
            remote(
                out.at[plane_z, q], fetched.at[plane_z, p], send.at[plane_z, q], recv.at[plane_z, p], at.device(z, q)
            ).start()
            return c

        lax.fori_loop(1, plane, start, 0)

    spread(z, panel)
    for k in range(1, line):
        for way in range(2):

            def pass_on(way=way, k=k):
                along(way, k).wait_recv()
                if k + 1 < line:
                    pl.when(sends(way, k + 1))(lambda: along(way, k + 1).start())

            pl.when(at.inside(source(way, k)))(pass_on)
        for way in range(2):
            pl.when(at.inside(source(way, k)))(
                lambda way=way, k=k: spread(source(way, k), unit(way, k))
            )
    for k in range(1, line):
        for way in range(2):
            pl.when(sends(way, k))(lambda way=way, k=k: along(way, k).wait_send())

    def finish(i, c):
        q = at.peer(i)
        for plane_z in range(line):
            remote(
                out.at[plane_z, q], fetched.at[plane_z, q], send.at[plane_z, q], recv.at[plane_z, q], at.device(z, q)
            ).wait()
        return c

    lax.fori_loop(1, plane, finish, 0)


def product_kernel(count, slot, row, tiles, fetched, sketch, outbound, sk, part):
    nslots = outbound.shape[0]
    steps = (count[0] + UNROLL - 1) // UNROLL

    def clear(ref):
        def body(i, c):
            ref[i] = jnp.zeros(ref.shape[1:], ref.dtype)
            return c

        lax.fori_loop(0, ref.shape[0], body, 0)

    clear(sk)
    clear(part)

    def forward(i, c):
        got = []
        for u in range(UNROLL):
            t = i * UNROLL + u
            block = fetched[jnp.minimum(slot[t], nslots - 1)]
            got.append(jnp.dot(tiles[t], block, preferred_element_type=jnp.float32))
        for u in range(UNROLL):
            r = row[i * UNROLL + u]
            sk[r] = sk[r] + got[u]
        return c

    lax.fori_loop(0, steps, forward, 0)

    def rounded(i, c):
        sketch[i] = sk[i].astype(sketch.dtype)
        return c

    lax.fori_loop(0, sketch.shape[0], rounded, 0)

    def backward(i, c):
        got = []
        for u in range(UNROLL):
            t = i * UNROLL + u
            block = sketch[jnp.minimum(row[t], sketch.shape[0] - 1)]
            got.append(
                lax.dot_general(
                    tiles[t], block, (((0,), (0,)), ((), ())), preferred_element_type=jnp.float32
                )
            )
        for u in range(UNROLL):
            s = slot[i * UNROLL + u]
            part[s] = part[s] + got[u]
        return c

    lax.fori_loop(0, steps, backward, 0)

    def send_form(i, c):
        outbound[i] = part[i].astype(outbound.dtype)
        return c

    lax.fori_loop(0, nslots, send_form, 0)


def reduce_kernel(line, rows, grp, ids, outbound, gram, inb, came, gone, total, z_send, z_recv, send, recv):
    at = Place(line, rows, grp)
    z, p, plane = at.z, at.p, at.plane
    held = gram.shape[0]
    at.greet()

    def target(way, k):
        return z + k if way == 0 else z - k

    def along(way, k):
        to = at.device(jnp.clip(target(way, 1), 0, line - 1), p)
        return remote(
            gone.at[way, k - 1], came.at[way, k - 1], z_send.at[way, k - 1], z_recv.at[way, k - 1], to
        )

    def begin(plane_z):
        def start(i, c):
            q = at.peer(i)
            remote(
                outbound.at[plane_z, q], inb.at[plane_z, p], send.at[plane_z, q], recv.at[plane_z, p], at.device(z, q)
            ).start()
            return c

        lax.fori_loop(1, plane, start, 0)
        for j in range(PAIR_CAP):
            inb[plane_z, p, j] = outbound[plane_z, p, j]

    def add_up(plane_z, into):
        def arrive(i, c):
            q = at.peer(i)
            remote(
                outbound.at[plane_z, q], inb.at[plane_z, q], send.at[plane_z, q], recv.at[plane_z, q], at.device(z, q)
            ).wait()
            return c

        lax.fori_loop(1, plane, arrive, 0)

        def block(b, c):
            def term(q, acc):
                for j in range(PAIR_CAP):
                    hit = ids[q, 0, plane_z * PAIR_CAP + j] == b
                    acc = acc + jnp.where(hit, inb[plane_z, q, j].astype(jnp.float32), 0.0)
                return acc

            zero = jnp.zeros(into.shape[1:], jnp.float32)
            into[b] = lax.fori_loop(0, plane, term, zero, unroll=8)
            return c

        lax.fori_loop(0, held, block, 0)

    stages = [(way, k) for k in range(line - 1, 0, -1) for way in range(2)]
    for way, k in stages:
        pl.when(at.inside(target(way, k)))(lambda way=way, k=k: begin(target(way, k)))
    begin(z)
    for k in range(line - 1, 0, -1):
        for way in range(2):
            pl.when(at.inside(target(way, k)))(
                lambda way=way, k=k: add_up(target(way, k), total.at[way])
            )
        for way in range(2):
            has = at.inside(target(way, -1))

            def joined(way=way, k=k):
                along(way, k + 1).wait_recv()

                def block(b, c):
                    gone[way, k - 1, b] = (
                        total[way, b] + came[way, k, b].astype(jnp.float32)
                    ).astype(gone.dtype)
                    return c

                lax.fori_loop(0, held, block, 0)

            def alone(way=way, k=k):
                def block(b, c):
                    gone[way, k - 1, b] = total[way, b].astype(gone.dtype)
                    return c

                lax.fori_loop(0, held, block, 0)

            def stage(way=way, k=k, has=has, joined=joined, alone=alone):
                if k + 1 < line:
                    pl.when(has)(joined)
                    pl.when(jnp.logical_not(has))(alone)
                else:
                    alone()
                along(way, k).start()

            pl.when(at.inside(target(way, k)))(stage)
    add_up(z, gram)
    for way in range(2):

        def last(way=way):
            along(way, 1).wait_recv()

            def block(b, c):
                gram[b] = gram[b] + came[way, 0, b].astype(jnp.float32)
                return c

            lax.fori_loop(0, held, block, 0)

        pl.when(at.inside(target(way, -1)))(last)
    for way, k in stages:
        pl.when(at.inside(target(way, k)))(lambda way=way, k=k: along(way, k).wait_send())


SMEM = pl.BlockSpec(memory_space=pltpu.SMEM)
VMEM = pl.BlockSpec(memory_space=pltpu.VMEM)
DMA = pltpu.SemaphoreType.DMA


def per_device(tiles, tile_rows, tile_cols, tile_count, block_perm, panel):
    rows, grp = lax.axis_size("rows"), lax.axis_size("grp")
    devices = rows * grp
    line = LINE if rows % LINE == 0 else rows
    plane = devices // line
    held, depth, width = panel.shape
    nslots = devices * PAIR_CAP
    part = width if nslots <= tiles.shape[0] else width // 2
    wanted, slot, row = index_tables(tile_rows, tile_cols, tile_count, block_perm, devices, held)
    by_peer = wanted.reshape(line, plane, PAIR_CAP).transpose(1, 0, 2).reshape(plane, 1, line * PAIR_CAP)
    by_peer = jnp.pad(by_peer, ((0, 0), (0, 7), (0, 128 - line * PAIR_CAP)))
    paired = (line, plane, PAIR_CAP, depth, width)
    unit = pltpu.VMEM(panel.shape, panel.dtype)
    params = pltpu.CompilerParams(vmem_limit_bytes=VMEM_LIMIT)
    fetched, asked = pl.pallas_call(
        functools.partial(fetch_kernel, line, rows, grp),
        out_shape=(
            jax.ShapeDtypeStruct(paired, panel.dtype),
            jax.ShapeDtypeStruct(by_peer.shape, jnp.int32),
        ),
        in_specs=[VMEM, VMEM],
        out_specs=(VMEM, VMEM),
        scratch_shapes=[unit] * (2 * (line - 1))
        + [
            pltpu.SMEM(by_peer.shape, jnp.int32),
            pltpu.VMEM(paired, panel.dtype),
            DMA((plane,)),
            DMA((plane,)),
            DMA((2, line - 1)),
            DMA((2, line - 1)),
            DMA((line, plane)),
            DMA((line, plane)),
            DMA(()),
        ],
        compiler_params=pltpu.CompilerParams(
            vmem_limit_bytes=VMEM_LIMIT, collective_id=0, has_side_effects=True
        ),
    )(by_peer, panel)
    sketch, outbound = pl.pallas_call(
        product_kernel,
        out_shape=(
            jax.ShapeDtypeStruct((RB_DEV, depth, width), jnp.bfloat16),
            jax.ShapeDtypeStruct((nslots, depth, width), jnp.bfloat16),
        ),
        grid=(width // part,),
        in_specs=[
            SMEM,
            SMEM,
            SMEM,
            pl.BlockSpec(tiles.shape, lambda k: (0, 0, 0), pipeline_mode=pl.Buffered(1)),
            pl.BlockSpec((nslots, depth, part), lambda k: (0, 0, k), pipeline_mode=pl.Buffered(1)),
        ],
        out_specs=(
            pl.BlockSpec((RB_DEV, depth, part), lambda k: (0, 0, k), pipeline_mode=pl.Buffered(1)),
            pl.BlockSpec((nslots, depth, part), lambda k: (0, 0, k), pipeline_mode=pl.Buffered(1)),
        ),
        scratch_shapes=[
            pltpu.VMEM((RB_DEV + 1, depth, part), jnp.float32),
            pltpu.VMEM((nslots + 1, depth, part), jnp.float32),
        ],
        compiler_params=params,
    )(tile_count, slot, row, tiles, fetched.reshape(nslots, depth, width))
    hops = pltpu.VMEM((2, line - 1) + panel.shape, jnp.bfloat16)
    gram = pl.pallas_call(
        functools.partial(reduce_kernel, line, rows, grp),
        out_shape=jax.ShapeDtypeStruct(panel.shape, jnp.float32),
        in_specs=[SMEM, VMEM],
        out_specs=VMEM,
        scratch_shapes=[
            pltpu.VMEM(paired, jnp.bfloat16),
            hops,
            hops,
            pltpu.VMEM((2,) + panel.shape, jnp.float32),
            DMA((2, line - 1)),
            DMA((2, line - 1)),
            DMA((line, plane)),
            DMA((line, plane)),
        ],
        compiler_params=pltpu.CompilerParams(
            vmem_limit_bytes=VMEM_LIMIT, collective_id=1, has_side_effects=True
        ),
    )(asked, outbound.reshape(paired))
    return sketch, gram


def solution(mesh):
    spec = P(AXES, None, None)
    return jax.shard_map(
        per_device,
        mesh=mesh,
        in_specs=(spec, P(AXES), P(AXES), P(AXES), P(), spec),
        out_specs=(spec, spec),
        check_vma=False,
    )
```

```python
import functools

import jax
import jax.numpy as jnp
from jax import lax
from jax.experimental import pallas as pl
from jax.experimental.pallas import tpu as pltpu
from jax.sharding import PartitionSpec as P

RB_DEV = 48
PAIR_CAP = 2
UNROLL = 4
CHUNKS = 4
AXES = ("rows", "grp")
VMEM_LIMIT = 60 * 1024 * 1024


def index_tables(tile_rows, tile_cols, tile_count, block_perm, devices, held):
    slots = tile_cols.shape[0]
    live = jnp.arange(slots, dtype=jnp.int32) < tile_count[0]
    blocks = jnp.arange(block_perm.shape[0], dtype=jnp.int32)
    stored = jnp.sum(jnp.where(tile_cols[:, None] == blocks[None, :], block_perm[None, :], 0), axis=1)
    owner = stored // held
    local = stored % held
    rank = jnp.any(
        live[None, :] & (owner[None, :] == owner[:, None]) & (local[None, :] < local[:, None]), axis=1
    ).astype(jnp.int32)
    mine = live[None, :] & (owner[None, :] == jnp.arange(devices, dtype=jnp.int32)[:, None])
    first = jnp.min(jnp.where(mine, local[None, :], held), axis=1)
    last = jnp.max(jnp.where(mine, local[None, :], -1), axis=1)
    wanted = jnp.stack(
        [jnp.where(last >= 0, first, -1), jnp.where(last > first, last, -1)], axis=-1
    ).astype(jnp.int32)
    slot = jnp.where(live, owner * PAIR_CAP + rank, devices * PAIR_CAP)
    row = jnp.where(live, tile_rows, RB_DEV)
    return wanted, slot.astype(jnp.int32), row.astype(jnp.int32)


LINE = 4
MESH = pl.DeviceIdType.MESH


class Place:
    def __init__(self, line, rows, grp):
        self.line, self.grp = line, grp
        self.plane_rows = rows // line
        self.plane = self.plane_rows * grp
        row = lax.axis_index("rows")
        self.z = row // self.plane_rows
        self.p = (row % self.plane_rows) * grp + lax.axis_index("grp")

    def device(self, z, p):
        return (z * self.plane_rows + p // self.grp, p % self.grp)

    def peer(self, i):
        return lax.rem(self.p + i, self.plane)

    def greet(self):
        barrier = pltpu.get_barrier_semaphore()
        for k in range(1, self.line):
            to = self.device(lax.rem(self.z + k, self.line), self.p)
            pl.semaphore_signal(barrier, inc=1, device_id=to, device_id_type=MESH)

        def signal(i, c):
            to = self.device(self.z, self.peer(i))
            pl.semaphore_signal(barrier, inc=1, device_id=to, device_id_type=MESH)
            return c

        lax.fori_loop(1, self.plane, signal, 0)
        pl.semaphore_wait(barrier, self.line - 1 + self.plane - 1)

    def inside(self, z):
        return (z >= 0) & (z < self.line)


def remote(src, dst, send, recv, to):
    return pltpu.make_async_remote_copy(
        src_ref=src, dst_ref=dst, send_sem=send, recv_sem=recv, device_id=to, device_id_type=MESH
    )


def fetch_kernel(line, rows, grp, wanted, panel, fetched, asked, *scratch):
    far, (ids, out, id_send, id_recv, z_send, z_recv, send, recv, local) = (
        scratch[: 2 * (line - 1) * CHUNKS],
        scratch[2 * (line - 1) * CHUNKS :],
    )
    at = Place(line, rows, grp)
    z, p, plane = at.z, at.p, at.plane
    at.greet()

    depth = panel.shape[1] // CHUNKS

    def part(n):
        return pl.ds(n * depth, depth)

    def unit(way, k, n):
        return panel.at[:, part(n)] if k == 0 else far[(way * (line - 1) + k - 1) * CHUNKS + n]

    def along(way, k, n):
        step = 1 if way == 0 else -1
        to = at.device(jnp.clip(z + step, 0, line - 1), p)
        sems = z_send.at[way, k - 1, n], z_recv.at[way, k - 1, n]
        return remote(unit(way, k - 1, n), unit(way, k, n), *sems, to)

    def source(way, k):
        return z - k if way == 0 else z + k

    def sends(way, k):
        return at.inside(z + (1 if way == 0 else -1)) & at.inside(source(way, k - 1))

    def id_copy(i, mine):
        q = at.peer(i)
        slot = p if mine else q
        return remote(wanted.at[q], asked.at[slot], id_send.at[q], id_recv.at[slot], at.device(z, q))

    def start_ids(i, c):
        id_copy(i, True).start()
        return c

    lax.fori_loop(1, plane, start_ids, 0)
    for n in range(CHUNKS):
        for way in range(2):
            pl.when(sends(way, 1))(lambda way=way, n=n: along(way, 1, n).start())
    asked[p] = wanted[p]

    def wait_ids(i, c):
        id_copy(i, False).wait()
        return c

    lax.fori_loop(1, plane, wait_ids, 0)
    to_smem = pltpu.make_async_copy(asked, ids, local)
    to_smem.start()
    to_smem.wait()

    def across(plane_z, q, n, slot):
        return remote(
            out.at[plane_z, n, q],
            fetched.at[plane_z, slot, :, part(n)],
            send.at[plane_z, n, q],
            recv.at[plane_z, n, slot],
            at.device(z, q),
        )

    def spread(plane_z, load, n):
        def pick(i, c):
            q = at.peer(i)
            for j in range(PAIR_CAP):
                out[plane_z, n, q, j] = load(jnp.maximum(ids[q, 0, plane_z * PAIR_CAP + j], 0))
            return c

        lax.fori_loop(1, plane, pick, 0)
        for j in range(PAIR_CAP):
            fetched[plane_z, p, j, part(n)] = load(
                jnp.maximum(ids[p, 0, plane_z * PAIR_CAP + j], 0)
            )

        def start(i, c):
            across(plane_z, at.peer(i), n, p).start()
            return c

        lax.fori_loop(1, plane, start, 0)

    for n in range(CHUNKS):
        spread(z, lambda block, n=n: panel[block, part(n)], n)
    for k, n in [(k, n) for k in range(1, line) for n in range(CHUNKS)]:
        for way in range(2):

            def pass_on(way=way, k=k, n=n):
                along(way, k, n).wait_recv()
                if k + 1 < line:
                    pl.when(sends(way, k + 1))(lambda: along(way, k + 1, n).start())

            pl.when(at.inside(source(way, k)))(pass_on)
        for way in range(2):

            def hand_out(way=way, k=k, n=n):
                held = unit(way, k, n)
                spread(source(way, k), lambda block: held[block], n)

            pl.when(at.inside(source(way, k)))(hand_out)
    for k, n in [(k, n) for k in range(1, line) for n in range(CHUNKS)]:
        for way in range(2):
            pl.when(sends(way, k))(lambda way=way, k=k, n=n: along(way, k, n).wait_send())

    def finish(i, c):
        q = at.peer(i)
        for plane_z in range(line):
            for n in range(CHUNKS):
                across(plane_z, q, n, q).wait()
        return c

    lax.fori_loop(1, plane, finish, 0)


def product_kernel(
    count, slot, row, tiles_in, fetched_in, sketch_out, outbound_out, tiles, fetched, sketch, outbound, sk, part, sem
):
    nslots, width = outbound.shape[0], outbound.shape[2]
    steps = (count[0] + UNROLL - 1) // UNROLL
    copy = pltpu.make_async_copy
    tile_copies = copy(tiles_in, tiles, sem.at[0])
    tile_copies.start()

    def clear(ref):
        def body(i, c):
            ref[i] = jnp.zeros(ref.shape[1:], ref.dtype)
            return c

        lax.fori_loop(0, ref.shape[0], body, 0)

    def forward(i, c):
        got = []
        for u in range(UNROLL):
            t = i * UNROLL + u
            block = fetched[jnp.minimum(slot[t], nslots - 1)]
            got.append(jnp.dot(tiles[t], block, preferred_element_type=jnp.float32))
        for u in range(UNROLL):
            r = row[i * UNROLL + u]
            sk[r] = sk[r] + got[u]
        return c

    def rounded(i, c):
        sketch[i] = sk[i].astype(sketch.dtype)
        return c

    def backward(i, c):
        got = []
        for u in range(UNROLL):
            t = i * UNROLL + u
            block = sketch[jnp.minimum(row[t], sketch.shape[0] - 1)]
            got.append(
                lax.dot_general(
                    tiles[t], block, (((0,), (0,)), ((), ())), preferred_element_type=jnp.float32
                )
            )
        for u in range(UNROLL):
            s = slot[i * UNROLL + u]
            part[s] = part[s] + got[u]
        return c

    for column in range(0, sketch_out.shape[2], width):
        columns = pl.ds(column, width)
        block_copies = copy(fetched_in.at[:, :, columns], fetched, sem.at[1])
        block_copies.start()
        clear(sk)
        clear(part)
        block_copies.wait()
        if column == 0:
            tile_copies.wait()
        lax.fori_loop(0, steps, forward, 0)
        lax.fori_loop(0, sketch.shape[0], rounded, 0)
        sketch_copies = copy(sketch, sketch_out.at[:, :, columns], sem.at[2])
        sketch_copies.start()
        lax.fori_loop(0, steps, backward, 0)
        group = nslots // 4
        out_copies = []
        for n in range(4):

            def send_form(i, c):
                outbound[i] = part[i].astype(outbound.dtype)
                return c

            lax.fori_loop(n * group, (n + 1) * group, send_form, 0)
            piece = pl.ds(n * group, group)
            out_copies.append(
                copy(outbound.at[piece], outbound_out.at[piece, :, columns], sem.at[3 + n])
            )
            out_copies[-1].start()
        sketch_copies.wait()
        for done in out_copies:
            done.wait()


def reduce_kernel(line, rows, grp, ids, outbound, gram, inb, came, gone, total, z_send, z_recv, send, recv):
    at = Place(line, rows, grp)
    z, p, plane = at.z, at.p, at.plane
    held = gram.shape[0]
    depth = gram.shape[1] // CHUNKS

    def part(n):
        return pl.ds(n * depth, depth)

    at.greet()

    def target(way, k):
        return z + k if way == 0 else z - k

    def along(way, k, n):
        to = at.device(jnp.clip(target(way, 1), 0, line - 1), p)
        return remote(
            gone.at[way, k - 1, n],
            came.at[way, k - 1, n],
            z_send.at[way, k - 1, n],
            z_recv.at[way, k - 1, n],
            to,
        )

    def across(plane_z, q, n, slot):
        return remote(
            outbound.at[plane_z, q, :, part(n)],
            inb.at[plane_z, n, slot],
            send.at[plane_z, n, q],
            recv.at[plane_z, n, slot],
            at.device(z, q),
        )

    def begin(plane_z, n):
        def start(i, c):
            across(plane_z, at.peer(i), n, p).start()
            return c

        lax.fori_loop(1, plane, start, 0)
        for j in range(PAIR_CAP):
            inb[plane_z, n, p, j] = outbound[plane_z, p, j, part(n)]

    def add_up(plane_z, n, into):
        def arrive(i, c):
            q = at.peer(i)
            across(plane_z, q, n, q).wait()
            return c

        lax.fori_loop(1, plane, arrive, 0)

        def block(b, c):
            def term(q, acc):
                for j in range(PAIR_CAP):
                    hit = ids[q, 0, plane_z * PAIR_CAP + j] == b
                    acc = acc + jnp.where(hit, inb[plane_z, n, q, j].astype(jnp.float32), 0.0)
                return acc

            zero = jnp.zeros((depth, gram.shape[2]), jnp.float32)
            into[b, part(n)] = lax.fori_loop(0, plane, term, zero, unroll=8)
            return c

        lax.fori_loop(0, held, block, 0)

    stages = [
        (way, k, n) for k in range(line - 1, 0, -1) for n in range(CHUNKS) for way in range(2)
    ]
    for way, k, n in stages:
        pl.when(at.inside(target(way, k)))(lambda way=way, k=k, n=n: begin(target(way, k), n))
    for n in range(CHUNKS):
        begin(z, n)
    for k, n in [(k, n) for k in range(line - 1, 0, -1) for n in range(CHUNKS)]:
        for way in range(2):
            pl.when(at.inside(target(way, k)))(
                lambda way=way, k=k, n=n: add_up(target(way, k), n, total.at[way])
            )
        for way in range(2):
            has = at.inside(target(way, -1))

            def joined(way=way, k=k, n=n):
                along(way, k + 1, n).wait_recv()

                def block(b, c):
                    gone[way, k - 1, n, b] = (
                        total[way, b, part(n)] + came[way, k, n, b].astype(jnp.float32)
                    ).astype(gone.dtype)
                    return c

                lax.fori_loop(0, held, block, 0)

            def alone(way=way, k=k, n=n):
                def block(b, c):
                    gone[way, k - 1, n, b] = total[way, b, part(n)].astype(gone.dtype)
                    return c

                lax.fori_loop(0, held, block, 0)

            def stage(way=way, k=k, n=n, has=has, joined=joined, alone=alone):
                if k + 1 < line:
                    pl.when(has)(joined)
                    pl.when(jnp.logical_not(has))(alone)
                else:
                    alone()
                along(way, k, n).start()

            pl.when(at.inside(target(way, k)))(stage)
    for n in range(CHUNKS):
        add_up(z, n, gram)
    for n in range(CHUNKS):
        for way in range(2):

            def last(way=way, n=n):
                along(way, 1, n).wait_recv()

                def block(b, c):
                    gram[b, part(n)] = gram[b, part(n)] + came[way, 0, n, b].astype(jnp.float32)
                    return c

                lax.fori_loop(0, held, block, 0)

            pl.when(at.inside(target(way, -1)))(last)
    for way, k, n in stages:
        pl.when(at.inside(target(way, k)))(lambda way=way, k=k, n=n: along(way, k, n).wait_send())


SMEM = pl.BlockSpec(memory_space=pltpu.SMEM)
VMEM = pl.BlockSpec(memory_space=pltpu.VMEM)
ANY = pl.BlockSpec(memory_space=pl.ANY)
DMA = pltpu.SemaphoreType.DMA


def per_device(tiles, tile_rows, tile_cols, tile_count, block_perm, panel):
    rows, grp = lax.axis_size("rows"), lax.axis_size("grp")
    devices = rows * grp
    line = LINE if rows % LINE == 0 else rows
    plane = devices // line
    held, depth, width = panel.shape
    nslots = devices * PAIR_CAP
    part = width if nslots <= tiles.shape[0] else width // 2
    wanted, slot, row = index_tables(tile_rows, tile_cols, tile_count, block_perm, devices, held)
    by_peer = wanted.reshape(line, plane, PAIR_CAP).transpose(1, 0, 2).reshape(plane, 1, line * PAIR_CAP)
    by_peer = jnp.pad(by_peer, ((0, 0), (0, 7), (0, 128 - line * PAIR_CAP)))
    paired = (line, plane, PAIR_CAP, depth, width)
    unit = pltpu.VMEM((held, depth // CHUNKS, width), panel.dtype)
    cut = (line, CHUNKS, plane, PAIR_CAP, depth // CHUNKS, width)
    params = pltpu.CompilerParams(vmem_limit_bytes=VMEM_LIMIT)
    fetched, asked = pl.pallas_call(
        functools.partial(fetch_kernel, line, rows, grp),
        out_shape=(
            jax.ShapeDtypeStruct(paired, panel.dtype),
            jax.ShapeDtypeStruct(by_peer.shape, jnp.int32),
        ),
        in_specs=[VMEM, VMEM],
        out_specs=(VMEM, VMEM),
        scratch_shapes=[unit] * (2 * (line - 1) * CHUNKS)
        + [
            pltpu.SMEM(by_peer.shape, jnp.int32),
            pltpu.VMEM(cut, panel.dtype),
            DMA((plane,)),
            DMA((plane,)),
            DMA((2, line - 1, CHUNKS)),
            DMA((2, line - 1, CHUNKS)),
            DMA((line, CHUNKS, plane)),
            DMA((line, CHUNKS, plane)),
            DMA(()),
        ],
        compiler_params=pltpu.CompilerParams(
            vmem_limit_bytes=VMEM_LIMIT, collective_id=0, has_side_effects=True
        ),
    )(by_peer, panel)
    sketch, outbound = pl.pallas_call(
        product_kernel,
        out_shape=(
            jax.ShapeDtypeStruct((RB_DEV, depth, width), jnp.bfloat16),
            jax.ShapeDtypeStruct((nslots, depth, width), jnp.bfloat16),
        ),
        in_specs=[SMEM, SMEM, SMEM, ANY, ANY],
        out_specs=(ANY, ANY),
        scratch_shapes=[
            pltpu.VMEM(tiles.shape, tiles.dtype),
            pltpu.VMEM((nslots, depth, part), panel.dtype),
            pltpu.VMEM((RB_DEV, depth, part), jnp.bfloat16),
            pltpu.VMEM((nslots, depth, part), jnp.bfloat16),
            pltpu.VMEM((RB_DEV + 1, depth, part), jnp.float32),
            pltpu.VMEM((nslots + 1, depth, part), jnp.float32),
            DMA((7,)),
        ],
        compiler_params=params,
    )(tile_count, slot, row, tiles, fetched.reshape(nslots, depth, width))
    hops = pltpu.VMEM((2, line - 1, CHUNKS, held, depth // CHUNKS, width), jnp.bfloat16)
    gram = pl.pallas_call(
        functools.partial(reduce_kernel, line, rows, grp),
        out_shape=jax.ShapeDtypeStruct(panel.shape, jnp.float32),
        in_specs=[SMEM, VMEM],
        out_specs=VMEM,
        scratch_shapes=[
            pltpu.VMEM(cut, jnp.bfloat16),
            hops,
            hops,
            pltpu.VMEM((2,) + panel.shape, jnp.float32),
            DMA((2, line - 1, CHUNKS)),
            DMA((2, line - 1, CHUNKS)),
            DMA((line, CHUNKS, plane)),
            DMA((line, CHUNKS, plane)),
        ],
        compiler_params=pltpu.CompilerParams(
            vmem_limit_bytes=VMEM_LIMIT, collective_id=1, has_side_effects=True
        ),
    )(asked, outbound.reshape(paired))
    return sketch, gram


def solution(mesh):
    spec = P(AXES, None, None)
    return jax.shard_map(
        per_device,
        mesh=mesh,
        in_specs=(spec, P(AXES), P(AXES), P(AXES), P(), spec),
        out_specs=(spec, spec),
        check_vma=False,
    )
```

```python
import functools

import jax
import jax.numpy as jnp
from jax import lax
from jax.experimental import pallas as pl
from jax.experimental.pallas import tpu as pltpu
from jax.sharding import PartitionSpec as P

RB_DEV = 48
PAIR_CAP = 2
UNROLL = 4
CHUNKS = 4
PIECES = 4
AXES = ("rows", "grp")
VMEM_LIMIT = 60 * 1024 * 1024


def index_tables(tile_rows, tile_cols, tile_count, block_perm, devices, held):
    slots = tile_cols.shape[0]
    live = jnp.arange(slots, dtype=jnp.int32) < tile_count[0]
    blocks = jnp.arange(block_perm.shape[0], dtype=jnp.int32)
    stored = jnp.sum(jnp.where(tile_cols[:, None] == blocks[None, :], block_perm[None, :], 0), axis=1)
    owner = stored // held
    local = stored % held
    rank = jnp.any(
        live[None, :] & (owner[None, :] == owner[:, None]) & (local[None, :] < local[:, None]), axis=1
    ).astype(jnp.int32)
    mine = live[None, :] & (owner[None, :] == jnp.arange(devices, dtype=jnp.int32)[:, None])
    first = jnp.min(jnp.where(mine, local[None, :], held), axis=1)
    last = jnp.max(jnp.where(mine, local[None, :], -1), axis=1)
    wanted = jnp.stack(
        [jnp.where(last >= 0, first, -1), jnp.where(last > first, last, -1)], axis=-1
    ).astype(jnp.int32)
    slot = jnp.where(live, owner * PAIR_CAP + rank, devices * PAIR_CAP)
    row = jnp.where(live, tile_rows, RB_DEV)
    return wanted, slot.astype(jnp.int32), row.astype(jnp.int32)


LINE = 4
MESH = pl.DeviceIdType.MESH


class Place:
    def __init__(self, line, rows, grp):
        self.line, self.grp = line, grp
        self.plane_rows = rows // line
        self.plane = self.plane_rows * grp
        row = lax.axis_index("rows")
        self.z = row // self.plane_rows
        self.p = (row % self.plane_rows) * grp + lax.axis_index("grp")

    def device(self, z, p):
        return (z * self.plane_rows + p // self.grp, p % self.grp)

    def peer(self, i):
        return lax.rem(self.p + i, self.plane)

    def greet(self):
        barrier = pltpu.get_barrier_semaphore()
        for k in range(1, self.line):
            to = self.device(lax.rem(self.z + k, self.line), self.p)
            pl.semaphore_signal(barrier, inc=1, device_id=to, device_id_type=MESH)

        def signal(i, c):
            to = self.device(self.z, self.peer(i))
            pl.semaphore_signal(barrier, inc=1, device_id=to, device_id_type=MESH)
            return c

        lax.fori_loop(1, self.plane, signal, 0)
        pl.semaphore_wait(barrier, self.line - 1 + self.plane - 1)

    def inside(self, z):
        return (z >= 0) & (z < self.line)


def remote(src, dst, send, recv, to):
    return pltpu.make_async_remote_copy(
        src_ref=src, dst_ref=dst, send_sem=send, recv_sem=recv, device_id=to, device_id_type=MESH
    )


def fetch_kernel(line, rows, grp, wanted, panel, fetched, asked, *scratch):
    far, (ids, out, id_send, id_recv, z_send, z_recv, send, recv, local) = (
        scratch[: 2 * (line - 1) * CHUNKS],
        scratch[2 * (line - 1) * CHUNKS :],
    )
    at = Place(line, rows, grp)
    z, p, plane = at.z, at.p, at.plane
    at.greet()

    depth = panel.shape[1] // CHUNKS

    def part(n):
        return pl.ds(n * depth, depth)

    def unit(way, k, n):
        return panel.at[:, part(n)] if k == 0 else far[(way * (line - 1) + k - 1) * CHUNKS + n]

    def along(way, k, n):
        step = 1 if way == 0 else -1
        to = at.device(jnp.clip(z + step, 0, line - 1), p)
        sems = z_send.at[way, k - 1, n], z_recv.at[way, k - 1, n]
        return remote(unit(way, k - 1, n), unit(way, k, n), *sems, to)

    def source(way, k):
        return z - k if way == 0 else z + k

    def sends(way, k):
        return at.inside(z + (1 if way == 0 else -1)) & at.inside(source(way, k - 1))

    def id_copy(i, mine):
        q = at.peer(i)
        slot = p if mine else q
        return remote(wanted.at[q], asked.at[slot], id_send.at[q], id_recv.at[slot], at.device(z, q))

    def start_ids(i, c):
        id_copy(i, True).start()
        return c

    lax.fori_loop(1, plane, start_ids, 0)
    for n in range(CHUNKS):
        for way in range(2):
            pl.when(sends(way, 1))(lambda way=way, n=n: along(way, 1, n).start())
    asked[p] = wanted[p]

    def wait_ids(i, c):
        id_copy(i, False).wait()
        return c

    lax.fori_loop(1, plane, wait_ids, 0)
    to_smem = pltpu.make_async_copy(asked, ids, local)
    to_smem.start()
    to_smem.wait()

    def across(plane_z, q, n, slot):
        return remote(
            out.at[plane_z, n, q],
            fetched.at[plane_z, slot, :, part(n)],
            send.at[plane_z, n, q],
            recv.at[plane_z, n, slot],
            at.device(z, q),
        )

    def keep(plane_z, n):
        return pltpu.make_async_copy(
            out.at[plane_z, n, p], fetched.at[plane_z, p, :, part(n)], send.at[plane_z, n, p]
        )

    def spread(plane_z, load, n):
        def pick(i, c):
            q = at.peer(i)
            for j in range(PAIR_CAP):
                out[plane_z, n, q, j] = load(jnp.maximum(ids[q, 0, plane_z * PAIR_CAP + j], 0))
            return c

        lax.fori_loop(1, plane, pick, 0)
        for j in range(PAIR_CAP):
            out[plane_z, n, p, j] = load(jnp.maximum(ids[p, 0, plane_z * PAIR_CAP + j], 0))

        def start(i, c):
            across(plane_z, at.peer(i), n, p).start()
            return c

        lax.fori_loop(1, plane, start, 0)
        keep(plane_z, n).start()

    for n in range(CHUNKS):
        spread(z, lambda block, n=n: panel[block, part(n)], n)
    for k, n in [(k, n) for k in range(1, line) for n in range(CHUNKS)]:
        for way in range(2):

            def pass_on(way=way, k=k, n=n):
                along(way, k, n).wait_recv()
                if k + 1 < line:
                    pl.when(sends(way, k + 1))(lambda: along(way, k + 1, n).start())

            pl.when(at.inside(source(way, k)))(pass_on)
        for way in range(2):

            def hand_out(way=way, k=k, n=n):
                held = unit(way, k, n)
                spread(source(way, k), lambda block: held[block], n)

            pl.when(at.inside(source(way, k)))(hand_out)
    for k, n in [(k, n) for k in range(1, line) for n in range(CHUNKS)]:
        for way in range(2):
            pl.when(sends(way, k))(lambda way=way, k=k, n=n: along(way, k, n).wait_send())

    def finish(i, c):
        q = at.peer(i)
        for plane_z in range(line):
            for n in range(CHUNKS):
                across(plane_z, q, n, q).wait()
        return c

    lax.fori_loop(1, plane, finish, 0)
    for plane_z in range(line):
        for n in range(CHUNKS):
            keep(plane_z, n).wait()


def product_kernel(
    count, slot, row, tiles_in, fetched_in, sketch_out, outbound_out, tiles, fetched, sketch, outbound, sk, part, sem
):
    nslots, width = outbound.shape[0], outbound.shape[2]
    steps = (count[0] + UNROLL - 1) // UNROLL
    copy = pltpu.make_async_copy
    group_steps = tiles.shape[0] // UNROLL // PIECES
    tile_copies = []
    for n in range(PIECES):
        piece = pl.ds(n * group_steps * UNROLL, group_steps * UNROLL)
        tile_copies.append(copy(tiles_in.at[piece], tiles.at[piece], sem.at[6 + n]))

    def clear(ref):
        def body(i, c):
            ref[i] = jnp.zeros(ref.shape[1:], ref.dtype)
            return c

        lax.fori_loop(0, ref.shape[0], body, 0)

    def forward(i, c):
        got = []
        for u in range(UNROLL):
            t = i * UNROLL + u
            block = fetched[jnp.minimum(slot[t], nslots - 1)]
            got.append(jnp.dot(tiles[t], block, preferred_element_type=jnp.float32))
        for u in range(UNROLL):
            r = row[i * UNROLL + u]
            sk[r] = sk[r] + got[u]
        return c

    def rounded(i, c):
        sketch[i] = sk[i].astype(sketch.dtype)
        return c

    def backward(i, c):
        got = []
        for u in range(UNROLL):
            t = i * UNROLL + u
            block = sketch[jnp.minimum(row[t], sketch.shape[0] - 1)]
            got.append(
                lax.dot_general(
                    tiles[t], block, (((0,), (0,)), ((), ())), preferred_element_type=jnp.float32
                )
            )
        for u in range(UNROLL):
            s = slot[i * UNROLL + u]
            part[s] = part[s] + got[u]
        return c

    for column in range(0, sketch_out.shape[2], width):
        columns = pl.ds(column, width)
        block_copies = copy(fetched_in.at[:, :, columns], fetched, sem.at[0])
        block_copies.start()
        if column == 0:
            for load in tile_copies:
                load.start()
        clear(sk)
        clear(part)
        block_copies.wait()
        for n in range(PIECES):
            if column == 0:
                tile_copies[n].wait()
            first = jnp.minimum(steps, n * group_steps)
            last = jnp.minimum(steps, (n + 1) * group_steps)
            lax.fori_loop(first, last, forward, 0)
        lax.fori_loop(0, sketch.shape[0], rounded, 0)
        sketch_copies = copy(sketch, sketch_out.at[:, :, columns], sem.at[1])
        sketch_copies.start()
        lax.fori_loop(0, steps, backward, 0)
        group = nslots // 4
        out_copies = []
        for n in range(4):

            def send_form(i, c):
                outbound[i] = part[i].astype(outbound.dtype)
                return c

            lax.fori_loop(n * group, (n + 1) * group, send_form, 0)
            piece = pl.ds(n * group, group)
            out_copies.append(
                copy(outbound.at[piece], outbound_out.at[piece, :, columns], sem.at[2 + n])
            )
            out_copies[-1].start()
        sketch_copies.wait()
        for done in out_copies:
            done.wait()


def reduce_kernel(line, rows, grp, ids, outbound, gram, inb, came, gone, total, z_send, z_recv, send, recv):
    at = Place(line, rows, grp)
    z, p, plane = at.z, at.p, at.plane
    held = gram.shape[0]
    depth = gram.shape[1] // CHUNKS

    def part(n):
        return pl.ds(n * depth, depth)

    at.greet()

    def target(way, k):
        return z + k if way == 0 else z - k

    def along(way, k, n):
        to = at.device(jnp.clip(target(way, 1), 0, line - 1), p)
        return remote(
            gone.at[way, k - 1, n],
            came.at[way, k - 1, n],
            z_send.at[way, k - 1, n],
            z_recv.at[way, k - 1, n],
            to,
        )

    def across(plane_z, q, n, slot):
        return remote(
            outbound.at[plane_z, q, :, part(n)],
            inb.at[plane_z, n, slot],
            send.at[plane_z, n, q],
            recv.at[plane_z, n, slot],
            at.device(z, q),
        )

    def keep(plane_z, n):
        return pltpu.make_async_copy(
            outbound.at[plane_z, p, :, part(n)], inb.at[plane_z, n, p], send.at[plane_z, n, p]
        )

    def begin(plane_z, n):
        def start(i, c):
            across(plane_z, at.peer(i), n, p).start()
            return c

        lax.fori_loop(1, plane, start, 0)
        keep(plane_z, n).start()

    def add_up(plane_z, n, into):
        def arrive(i, c):
            q = at.peer(i)
            across(plane_z, q, n, q).wait()
            return c

        lax.fori_loop(1, plane, arrive, 0)
        keep(plane_z, n).wait()

        def block(b, c):
            def term(q, acc):
                for j in range(PAIR_CAP):
                    hit = ids[q, 0, plane_z * PAIR_CAP + j] == b
                    acc = acc + jnp.where(hit, inb[plane_z, n, q, j].astype(jnp.float32), 0.0)
                return acc

            zero = jnp.zeros((depth, gram.shape[2]), jnp.float32)
            into[b, part(n)] = lax.fori_loop(0, plane, term, zero, unroll=8)
            return c

        lax.fori_loop(0, held, block, 0)

    stages = [
        (way, k, n) for k in range(line - 1, 0, -1) for n in range(CHUNKS) for way in range(2)
    ]
    for way, k, n in stages:
        pl.when(at.inside(target(way, k)))(lambda way=way, k=k, n=n: begin(target(way, k), n))
    for n in range(CHUNKS):
        begin(z, n)
    for k, n in [(k, n) for k in range(line - 1, 0, -1) for n in range(CHUNKS)]:
        for way in range(2):
            pl.when(at.inside(target(way, k)))(
                lambda way=way, k=k, n=n: add_up(target(way, k), n, total.at[way])
            )
        for way in range(2):
            has = at.inside(target(way, -1))

            def joined(way=way, k=k, n=n):
                along(way, k + 1, n).wait_recv()

                def block(b, c):
                    gone[way, k - 1, n, b] = (
                        total[way, b, part(n)] + came[way, k, n, b].astype(jnp.float32)
                    ).astype(gone.dtype)
                    return c

                lax.fori_loop(0, held, block, 0)

            def alone(way=way, k=k, n=n):
                def block(b, c):
                    gone[way, k - 1, n, b] = total[way, b, part(n)].astype(gone.dtype)
                    return c

                lax.fori_loop(0, held, block, 0)

            def stage(way=way, k=k, n=n, has=has, joined=joined, alone=alone):
                if k + 1 < line:
                    pl.when(has)(joined)
                    pl.when(jnp.logical_not(has))(alone)
                else:
                    alone()
                along(way, k, n).start()

            pl.when(at.inside(target(way, k)))(stage)
    for n in range(CHUNKS):
        add_up(z, n, gram)
    for n in range(CHUNKS):
        for way in range(2):

            def last(way=way, n=n):
                along(way, 1, n).wait_recv()

                def block(b, c):
                    gram[b, part(n)] = gram[b, part(n)] + came[way, 0, n, b].astype(jnp.float32)
                    return c

                lax.fori_loop(0, held, block, 0)

            pl.when(at.inside(target(way, -1)))(last)
    for way, k, n in stages:
        pl.when(at.inside(target(way, k)))(lambda way=way, k=k, n=n: along(way, k, n).wait_send())


SMEM = pl.BlockSpec(memory_space=pltpu.SMEM)
VMEM = pl.BlockSpec(memory_space=pltpu.VMEM)
ANY = pl.BlockSpec(memory_space=pl.ANY)
DMA = pltpu.SemaphoreType.DMA


def per_device(tiles, tile_rows, tile_cols, tile_count, block_perm, panel):
    rows, grp = lax.axis_size("rows"), lax.axis_size("grp")
    devices = rows * grp
    line = LINE if rows % LINE == 0 else rows
    plane = devices // line
    held, depth, width = panel.shape
    nslots = devices * PAIR_CAP
    part = width if nslots <= tiles.shape[0] else width // 2
    wanted, slot, row = index_tables(tile_rows, tile_cols, tile_count, block_perm, devices, held)
    by_peer = wanted.reshape(line, plane, PAIR_CAP).transpose(1, 0, 2).reshape(plane, 1, line * PAIR_CAP)
    by_peer = jnp.pad(by_peer, ((0, 0), (0, 7), (0, 128 - line * PAIR_CAP)))
    paired = (line, plane, PAIR_CAP, depth, width)
    unit = pltpu.VMEM((held, depth // CHUNKS, width), panel.dtype)
    cut = (line, CHUNKS, plane, PAIR_CAP, depth // CHUNKS, width)
    params = pltpu.CompilerParams(vmem_limit_bytes=VMEM_LIMIT)
    fetched, asked = pl.pallas_call(
        functools.partial(fetch_kernel, line, rows, grp),
        out_shape=(
            jax.ShapeDtypeStruct(paired, panel.dtype),
            jax.ShapeDtypeStruct(by_peer.shape, jnp.int32),
        ),
        in_specs=[VMEM, VMEM],
        out_specs=(ANY, VMEM),
        scratch_shapes=[unit] * (2 * (line - 1) * CHUNKS)
        + [
            pltpu.SMEM(by_peer.shape, jnp.int32),
            pltpu.VMEM(cut, panel.dtype),
            DMA((plane,)),
            DMA((plane,)),
            DMA((2, line - 1, CHUNKS)),
            DMA((2, line - 1, CHUNKS)),
            DMA((line, CHUNKS, plane)),
            DMA((line, CHUNKS, plane)),
            DMA(()),
        ],
        compiler_params=pltpu.CompilerParams(
            vmem_limit_bytes=VMEM_LIMIT, collective_id=0, has_side_effects=True
        ),
    )(by_peer, panel)
    sketch, outbound = pl.pallas_call(
        product_kernel,
        out_shape=(
            jax.ShapeDtypeStruct((RB_DEV, depth, width), jnp.bfloat16),
            jax.ShapeDtypeStruct((nslots, depth, width), jnp.bfloat16),
        ),
        in_specs=[SMEM, SMEM, SMEM, ANY, ANY],
        out_specs=(ANY, ANY),
        scratch_shapes=[
            pltpu.VMEM(tiles.shape, tiles.dtype),
            pltpu.VMEM((nslots, depth, part), panel.dtype),
            pltpu.VMEM((RB_DEV, depth, part), jnp.bfloat16),
            pltpu.VMEM((nslots, depth, part), jnp.bfloat16),
            pltpu.VMEM((RB_DEV + 1, depth, part), jnp.float32),
            pltpu.VMEM((nslots + 1, depth, part), jnp.float32),
            DMA((6 + PIECES,)),
        ],
        compiler_params=params,
    )(tile_count, slot, row, tiles, fetched.reshape(nslots, depth, width))
    hops = pltpu.VMEM((2, line - 1, CHUNKS, held, depth // CHUNKS, width), jnp.bfloat16)
    gram = pl.pallas_call(
        functools.partial(reduce_kernel, line, rows, grp),
        out_shape=jax.ShapeDtypeStruct(panel.shape, jnp.float32),
        in_specs=[SMEM, ANY],
        out_specs=VMEM,
        scratch_shapes=[
            pltpu.VMEM(cut, jnp.bfloat16),
            hops,
            hops,
            pltpu.VMEM((2,) + panel.shape, jnp.float32),
            DMA((2, line - 1, CHUNKS)),
            DMA((2, line - 1, CHUNKS)),
            DMA((line, CHUNKS, plane)),
            DMA((line, CHUNKS, plane)),
        ],
        compiler_params=pltpu.CompilerParams(
            vmem_limit_bytes=VMEM_LIMIT, collective_id=1, has_side_effects=True
        ),
    )(asked, outbound.reshape(paired))
    return sketch, gram


def solution(mesh):
    spec = P(AXES, None, None)
    return jax.shard_map(
        per_device,
        mesh=mesh,
        in_specs=(spec, P(AXES), P(AXES), P(AXES), P(), spec),
        out_specs=(spec, spec),
        check_vma=False,
    )
```
